256 devices in a mesh: arcs: 2 (over z_lo), trow: 8 (over y, core), tcol: 16 (over x, z_hi).
Axes of the slice: x: 4, y: 4, z: 8 (z_hi: 4, z_lo: 2; z = z_hi * 2 + z_lo), core: 2. Of those that a mesh axis runs over, the one named last changes fastest.
Arguments:
- design: bfloat16 [4096, 12288], P(('arcs', 'tcol'), 'trow'), may hold values from -6 to 6
- observed: float32 [4096], P(('arcs', 'tcol')), may hold values from -6 to 6
- arc_counts: int32 [128], P(('arcs', 'tcol')), may hold values from 2 to 32
- arc_weight: float32 [128], P(('arcs', 'tcol')), may hold values from 0.3 to 3
Outputs:
- gram: float32 [12288, 12288], P('trow', ('arcs', 'tcol'))
- rhs: float32 [12288], P('trow')
The draws below stay inside these ranges and needn't reach their ends.
Inputs may be any that keep to these rules, and one draw needn't show every extreme that they name: `arc_counts`: each arc has at least two valid observations.
All inputs are finite; a program needn't handle non-finite values.
Results may differ from the reference program's by a relative error of at most 0.0055.
Values may be sent and summed in bfloat16 or wider, within the bound.
No kernel may reach another device: no remote copies, remote signals or barrier semaphores. Data moves between devices by JAX's collectives and lax.ppermute only.
A program may use at most 192 MiB of HBM per device.

```python
import math
import jax
import jax.numpy as jnp
from jax import lax

K = 12288
ARC_LEN = 32
OBS = 4096
ARCS = 128


def plant(values, key, least, largest):
    index_at = [jax.random.randint(jax.random.fold_in(key, axis), (), 0, length) for axis, length in enumerate(values.shape)]
    longest = values.shape.index(max(values.shape))
    beside = index_at[:longest] + [(index_at[longest] + 1) % values.shape[longest]] + index_at[longest + 1:]
    return values.at[tuple(index_at)].set(least).at[tuple(beside)].set(largest)


def levels(own_key, extent, shards, least, largest):
    level = 1.0
    for position, blocks in shards:
        steps = jax.random.uniform(jax.random.fold_in(jax.random.fold_in(own_key, 6), position), (blocks,), jnp.float32, least / len(shards), largest / len(shards))
        level = level * jnp.repeat(jnp.exp(steps), extent[position] // blocks).reshape((-1,) + (1,) * (len(extent) - 1 - position))
    return level


def normal_values(rng, extent, spread, limit, pieces=(), held_as=jnp.bfloat16):
    level = levels(rng, extent, pieces, -0.22, 0.18) if pieces else 1.0
    entries = jax.random.normal(rng, extent, jnp.float32) * spread * level
    return jnp.minimum(jnp.maximum(entries, -limit), limit).astype(held_as)


def setup_inputs(seed: int = 0) -> dict:
    key_list = jax.random.split(jax.random.key(seed), 5)
    return {
        "design": normal_values(key_list[0], (OBS, K), 1.0, 6.0, ((0, 32), (1, 8))),
        "observed": normal_values(key_list[1], (OBS,), 1.0, 6.0, ((0, 32),), jnp.float32),
        "arc_counts": plant(jax.random.randint(key_list[2], (ARCS,), 2, ARC_LEN + 1), jax.random.fold_in(key_list[2], 1), 2, ARC_LEN).astype(jnp.int32),
        "arc_weight": jnp.clip(jnp.exp(math.log(3.0) - 2.3025851 * jax.random.uniform(key_list[3], (ARCS,), jnp.float32) ** levels(key_list[3], (ARCS,), ((0, 32),), -0.2, 0.2)), 0.3, 3.0),
    }


def reference(design, observed, arc_counts, arc_weight):
    obs_count, col_width = design.shape
    arc_total = arc_counts.shape[0]
    arc_len = obs_count // arc_total
    slot_index = lax.broadcasted_iota(jnp.int32, (arc_total, arc_len), 1)
    valid_mask = (slot_index < arc_counts[:, None]).astype(jnp.float32)
    counts_float = arc_counts.astype(jnp.float32)
    factor = valid_mask * jnp.sqrt(arc_weight)[:, None]
    blocks = design.reshape(arc_total, arc_len, col_width).astype(jnp.float32)
    column_mean = lax.optimization_barrier(jnp.sum(valid_mask[:, :, None] * blocks, axis=1)) / counts_float[:, None]
    centered = (factor[:, :, None] * (blocks - column_mean[:, None, :])).reshape(obs_count, col_width).astype(jnp.bfloat16)
    series = observed.reshape(arc_total, arc_len)
    series_mean = lax.optimization_barrier(jnp.sum(valid_mask * series, axis=1)) / counts_float
    weighted = (factor * (series - series_mean[:, None])).reshape(obs_count)
    widened = centered.astype(jnp.float32)
    gram = jnp.dot(widened.T, widened, precision=lax.Precision.HIGHEST, preferred_element_type=jnp.float32) * (1.0 / obs_count)
    rhs = jnp.dot(weighted, widened, precision=lax.Precision.HIGHEST) * obs_count ** (-0.5)
    return (gram, rhs)
```

```python
import jax
import jax.numpy as jnp
from jax import lax
from jax.experimental import pallas as pl
from jax.experimental.pallas import tpu as pltpu
from jax.sharding import PartitionSpec as P


AXES = ("arcs", "trow", "tcol")
CHUNKS = 3


def device_index(x, y, core, zh, zl):
    return (zl * 8 + y * 2 + core) * 16 + x * 4 + zh


def moved(value, where):
    pairs = []
    for x in range(4):
        for y in range(4):
            for core in range(2):
                for zh in range(4):
                    for zl in range(2):
                        pairs.append(
                            (device_index(x, y, core, zh, zl), device_index(*where(x, y, core, zh, zl)))
                        )
    return lax.ppermute(value, AXES, pairs)


def along_z(value, step):
    def where(x, y, core, zh, zl):
        z = (zh * 2 + zl + step) % 8
        return x, y, core, z // 2, z % 2

    return moved(value, where)


def flip_z(value, mask):
    def where(x, y, core, zh, zl):
        z = (zh * 2 + zl) ^ mask
        return x, y, core, z // 2, z % 2

    return moved(value, where)


def flip_x(value, mask):
    return moved(value, lambda x, y, core, zh, zl: (x ^ mask, y, core, zh, zl))


def along_y(value, step):
    return moved(value, lambda x, y, core, zh, zl: (x, (y + step) % 4, core, zh, zl))


def flip_core(value):
    return moved(value, lambda x, y, core, zh, zl: (x, y, 1 - core, zh, zl))


def to_share(value, turn):
    def where(x, y, core, zh, zl):
        a = y // 2
        return x, (y if zl == a else 3 - y), core, (zh + turn) % 4, a

    return moved(value, where)


def place_columns(where_ref, *refs):
    out_ref = refs[-1]
    x, y, core, zl = (where_ref[i] for i in range(4))
    for other in range(2):
        own, up1, down1, up2, down2 = refs[5 * other : 5 * other + 5]
        for turn in range(4):
            two = up2 if turn < 2 else down2
            sources = (own[turn], down1[turn], two[turn % 2], up1[turn])
            for y_rel, piece in enumerate(sources):
                q = (y + y_rel + 6 * zl) % 4
                j = jnp.where((q == 1) | (q == 2), 1, 0)
                side = q // 2
                block = (2 * j + (core + other) % 2) ^ x
                obs = jnp.where(side == 0, turn, 4 + (turn + zl) % 4)
                out_ref[block, pl.ds(pl.multiple_of(obs * 128, 128), 128), :] = piece


def columns_of(where, parts):
    return pl.pallas_call(
        place_columns,
        out_shape=jax.ShapeDtypeStruct((4, 1024, 384), jnp.bfloat16),
        in_specs=[pl.BlockSpec(memory_space=pltpu.SMEM)]
        + [pl.BlockSpec(memory_space=pltpu.VMEM)] * len(parts),
        out_specs=pl.BlockSpec(memory_space=pltpu.VMEM),
        name="place_columns",
    )(where, *parts)


def product(left, right):
    return lax.dot_general(left, right, (((0,), (0,)), ((), ())), preferred_element_type=jnp.float32)


def ring_rows(piece):
    up, down = piece, piece
    ups, downs = [], []
    for _ in range(3):
        up, down = along_z(up, 1), along_z(down, -1)
        ups.append(up)
        downs.append(down)
    half = piece.shape[0] // 2
    far = [along_z(up[:half], 1), along_z(down[half:], -1)]
    return jnp.concatenate(
        [piece, ups[1], *far, downs[1], downs[0], ups[0], ups[2], downs[2]], axis=0
    )


def local(design, observed, arc_counts, arc_weight):
    row_count, col_width = design.shape
    arc_total = arc_counts.shape[0]
    arc_len = row_count // arc_total
    slot_index = lax.broadcasted_iota(jnp.int32, (arc_total, arc_len), 1)
    valid_mask = (slot_index < arc_counts[:, None]).astype(jnp.float32)
    counts_float = arc_counts.astype(jnp.float32)
    factor = valid_mask * jnp.sqrt(arc_weight)[:, None]
    blocks = design.reshape(arc_total, arc_len, col_width).astype(jnp.float32)
    column_mean = jnp.sum(valid_mask[:, :, None] * blocks, axis=1) / counts_float[:, None]
    centered = (
        (factor[:, :, None] * (blocks - column_mean[:, None, :]))
        .reshape(row_count, col_width)
        .astype(jnp.bfloat16)
    )
    series = observed.reshape(arc_total, arc_len)
    series_mean = jnp.sum(valid_mask * series, axis=1) / counts_float
    weighted = (factor * (series - series_mean[:, None])).reshape(row_count)
    obs_total = 4096

    zl = lax.axis_index("arcs")
    trow = lax.axis_index("trow")
    tcol = lax.axis_index("tcol")
    x, zh, y, core = tcol // 4, tcol % 4, trow // 2, trow % 2

    narrow = col_width // 4
    shares = []
    for turn in range(4):
        start = ((zh + turn) % 4) * narrow
        shares.append(to_share(lax.dynamic_slice(centered, (0, start), (row_count, narrow)), turn))
    share = jnp.stack(shares)
    up1, down1 = along_y(share, 1), along_y(share, -1)
    up2, down2 = along_y(up1[:2], 1), along_y(down1[2:], -1)
    mine = [share, up1, down1, up2, down2]
    right = columns_of(jnp.stack([x, y, core, zl]), mine + [flip_core(v) for v in mine])

    width = col_width // CHUNKS
    half = width // 2
    send_p = jnp.concatenate([right[1], right[2]], axis=1)
    send_q = jnp.concatenate([right[2], right[3]], axis=1)
    tiles = []
    for c in range(CHUNKS):
        rows = ring_rows(centered[:, c * width : (c + 1) * width])
        first, second = rows[:, :half], rows[:, half:]
        got = flip_x(product(first, send_p).astype(jnp.bfloat16), 1)
        own = product(first, right[0]) + got[:, :narrow].astype(jnp.float32)
        on = product(first, right[3]) + got[:, narrow:].astype(jnp.float32)
        last = flip_x(on.astype(jnp.bfloat16), 3)
        tiles.append((own + last.astype(jnp.float32)) * (1.0 / obs_total))
        got = flip_x(product(second, send_q).astype(jnp.bfloat16), 3)
        own = product(second, right[0]) + got[:, narrow:].astype(jnp.float32)
        on = product(second, right[1]) + got[:, :narrow].astype(jnp.float32)
        last = flip_x(on.astype(jnp.bfloat16), 1)
        tiles.append((own + last.astype(jnp.float32)) * (1.0 / obs_total))
    gram = jnp.concatenate(tiles, axis=0)

    rhs = jnp.dot(weighted, centered.astype(jnp.float32), precision=lax.Precision.HIGHEST)
    for mask in (1, 2, 4):
        rhs = rhs + flip_z(rhs, mask)
    for mask in (1, 3):
        rhs = rhs + flip_x(rhs, mask)
    return (gram, rhs * obs_total ** (-0.5))


def solution(mesh):
    return jax.shard_map(
        local,
        mesh=mesh,
        in_specs=(
            P(("arcs", "tcol"), "trow"),
            P(("arcs", "tcol")),
            P(("arcs", "tcol")),
            P(("arcs", "tcol")),
        ),
        out_specs=(P("trow", ("arcs", "tcol")), P("trow")),
        check_vma=False,
    )
```

```python
import jax
import jax.numpy as jnp
from jax import lax
from jax.experimental import pallas as pl
from jax.experimental.pallas import tpu as pltpu
from jax.sharding import PartitionSpec as P


AXES = ("arcs", "trow", "tcol")


def device_index(x, y, core, zh, zl):
    return (zl * 8 + y * 2 + core) * 16 + x * 4 + zh


def moved(value, where):
    pairs = []
    for x in range(4):
        for y in range(4):
            for core in range(2):
                for zh in range(4):
                    for zl in range(2):
                        pairs.append(
                            (device_index(x, y, core, zh, zl), device_index(*where(x, y, core, zh, zl)))
                        )
    return lax.ppermute(value, AXES, pairs)


def along_z(step):
    def where(x, y, core, zh, zl):
        z = (zh * 2 + zl + step) % 8
        return x, y, core, z // 2, z % 2

    return where


def round_y(x, y, core, zh, zl):
    return x, (y + (1 if core == 0 else 3)) % 4, core, zh, zl


def other_core(x, y, core, zh, zl):
    return x, y, 1 - core, zh, zl


def first_x(x, y, core, zh, zl):
    return x ^ (1 if core == 0 else 3), y, core, zh, zl


def second_x(x, y, core, zh, zl):
    return x ^ (3 if core == 0 else 1), y, core, zh, zl


def flip_z(mask):
    def where(x, y, core, zh, zl):
        z = (zh * 2 + zl) ^ mask
        return x, y, core, z // 2, z % 2

    return where


def to_share(turn):
    def where(x, y, core, zh, zl):
        a = y // 2
        return x, (y if zl == a else 3 - y), core, (zh + turn) % 4, a

    return where


def centre(where_ref, *refs):
    sources, out_ref, share_refs, rhs_ref = refs[:4], refs[4], refs[5:9], refs[9]
    counts_ref, weight_ref, design_ref, observed_ref = refs[10:14]
    copies = [pltpu.make_async_copy(sources[i], refs[10 + i], refs[14].at[i]) for i in range(4)]
    for copy in copies:
        copy.start()
    for copy in copies:
        copy.wait()
    arcs = counts_ref.shape[0]
    rows, cols = design_ref.shape
    length = rows // arcs
    slot = lax.broadcasted_iota(jnp.int32, (length, 1), 0)
    lane = lax.broadcasted_iota(jnp.int32, (1, rows), 1)
    observed = observed_ref[...]
    weighted = jnp.zeros((1, rows), jnp.float32)
    for arc in range(arcs):
        count = counts_ref[arc]
        mask = (slot < count).astype(jnp.float32)
        total = jnp.full((1, 1), count.astype(jnp.float32))
        root = jnp.sqrt(jnp.full((1, 1), weight_ref[arc]))
        piece = design_ref[pl.ds(arc * length, length), :].astype(jnp.float32)
        mean = jnp.sum(mask * piece, axis=0, keepdims=True) / total
        out_ref[pl.ds(arc * length, length), :] = ((mask * root) * (piece - mean)).astype(jnp.bfloat16)
        inside = ((lane >= arc * length) & (lane < arc * length + count)).astype(jnp.float32)
        series_mean = jnp.sum(inside * observed, axis=1, keepdims=True) / total
        weighted = weighted + (inside * root) * (observed - series_mean)
    high = weighted.astype(jnp.bfloat16)
    rest1 = weighted - high.astype(jnp.float32)
    middle = rest1.astype(jnp.bfloat16)
    low = (rest1 - middle.astype(jnp.float32)).astype(jnp.bfloat16)
    row = lax.broadcasted_iota(jnp.int32, (8, rows), 0)
    parts = jnp.where(
        row == 0,
        high.astype(jnp.float32),
        jnp.where(row == 1, middle.astype(jnp.float32), jnp.where(row == 2, low.astype(jnp.float32), 0.0)),
    ).astype(jnp.bfloat16)
    sums = jnp.dot(parts, out_ref[...], preferred_element_type=jnp.float32)
    rhs_ref[...] = jnp.sum(sums, axis=0, keepdims=True)
    narrow = cols // 4
    for turn, share_ref in enumerate(share_refs):
        start = pl.multiple_of(((where_ref[3] + turn) % 4) * narrow, 128)
        share_ref[...] = out_ref[:, pl.ds(start, narrow)]


def place(where_ref, *refs):
    rows_refs, column_refs, rows_out, cols_out = refs[:9], refs[9:-2], refs[-2], refs[-1]
    x, y, core, zh, zl = (where_ref[i] for i in range(5))
    start = 0
    for ref in rows_refs:
        rows_out[pl.ds(start, ref.shape[0]), :] = ref[...]
        start += ref.shape[0]
    z = 2 * zh + zl
    behind = jnp.where(core == 0, 3, 1)
    first = jnp.where(core == 0, 1, 3)

    def put(source_core, offset, ref):
        from_y = (y + offset) % 4
        near = from_y // 2 == zl
        of_y = jnp.where(near, from_y, 3 - from_y)
        of_zl = jnp.where(near, zl, 1 - zl)
        m = (2 * (of_y % 2) + source_core) ^ x
        spot = jnp.where(m == 0, 0, jnp.where(m == 2, 3, jnp.where(m == first, 2, 1)))
        for turn in range(4):
            of_z = 2 * ((zh + 4 - turn) % 4) + of_zl
            ahead = (of_z + 8 - z) % 8
            cols_out[
                spot // 2,
                pl.ds(pl.multiple_of(ahead * 128, 128), 128),
                pl.ds(pl.multiple_of((spot % 2) * 384, 128), 384),
            ] = ref[turn]

    share, c0, y1, y1c, c1, c1c, y2, c2 = column_refs
    put(core, 0, share)
    put(1 - core, 0, c0)
    put(core, behind, y1)
    put(1 - core, behind, y1c)
    put(1 - core, 4 - behind, c1)
    put(core, 4 - behind, c1c)
    put(core, 2, y2)
    put(1 - core, 2, c2)


def product(left, right):
    return lax.dot_general(left, right, (((0,), (0,)), ((), ())), preferred_element_type=jnp.float32)


VMEM = pl.BlockSpec(memory_space=pltpu.VMEM)
SMEM = pl.BlockSpec(memory_space=pltpu.SMEM)


def local(design, observed, arc_counts, arc_weight):
    rows, cols = design.shape
    narrow = cols // 4
    obs_total = 4096
    bf16, f32 = jnp.bfloat16, jnp.float32
    trow, tcol = lax.axis_index("trow"), lax.axis_index("tcol")
    where = jnp.stack([tcol // 4, trow // 2, trow % 2, tcol % 4, lax.axis_index("arcs")])

    out = pl.pallas_call(
        centre,
        out_shape=[jax.ShapeDtypeStruct((rows, cols), bf16)]
        + [jax.ShapeDtypeStruct((rows, narrow), bf16)] * 4
        + [jax.ShapeDtypeStruct((1, cols), f32)],
        in_specs=[SMEM] + [pl.BlockSpec(memory_space=pltpu.HBM)] * 4,
        out_specs=[VMEM] * 6,
        scratch_shapes=[
            pltpu.SMEM(arc_counts.shape, arc_counts.dtype),
            pltpu.SMEM(arc_weight.shape, arc_weight.dtype),
            pltpu.VMEM(design.shape, design.dtype),
            pltpu.VMEM((1, rows), f32),
            pltpu.SemaphoreType.DMA((4,)),
        ],
        compiler_params=pltpu.CompilerParams(vmem_limit_bytes=8 << 20),
        name="centre",
    )(where, arc_counts, arc_weight, design, observed.reshape(1, rows))
    centered, shares, rhs = out[0], out[1:5], out[5].reshape(cols)

    up, down = [centered], [centered]
    for _ in range(1, 4):
        up.append(moved(up[-1], along_z(1)))
        down.append(moved(down[-1], along_z(-1)))
    far_up = moved(up[3][: rows // 2], along_z(1))
    far_down = moved(down[3][rows // 2 :], along_z(-1))
    pieces = [centered, *down[1:], far_up, far_down, up[3], up[2], up[1]]

    share = jnp.concatenate([moved(shares[turn], to_share(turn))[None] for turn in range(4)])
    c0 = moved(share, other_core)
    y1, y1c = moved(share, round_y), moved(c0, round_y)
    c1, c1c = moved(y1, other_core), moved(y1c, other_core)
    y2 = moved(y1, round_y)
    columns = [share, c0, y1, y1c, c1, c1c, y2, moved(y2, other_core)]

    every_row, right = pl.pallas_call(
        place,
        out_shape=[
            jax.ShapeDtypeStruct((8 * rows, cols), bf16),
            jax.ShapeDtypeStruct((2, 8 * rows, 2 * narrow), bf16),
        ],
        in_specs=[SMEM] + [VMEM] * 17,
        out_specs=[VMEM] * 2,
        compiler_params=pltpu.CompilerParams(vmem_limit_bytes=20 << 20),
        name="place",
    )(where, *pieces, *columns)

    send = product(every_row, right[1]).astype(bf16)
    got = moved(send, first_x).astype(f32)
    keep = lax.optimization_barrier(product(every_row, right[0]))
    last = moved((keep[:, narrow:] + got[:, narrow:]).astype(bf16), second_x)
    gram = (keep[:, :narrow] + got[:, :narrow] + last.astype(f32)) * (1.0 / obs_total)

    for mask in (1, 2, 4):
        rhs = rhs + moved(rhs, flip_z(mask))
    rhs = rhs + moved(rhs, second_x)
    rhs = rhs + moved(rhs, first_x)
    return (gram, rhs * obs_total ** (-0.5))


def solution(mesh):
    return jax.shard_map(
        local,
        mesh=mesh,
        in_specs=(
            P(("arcs", "tcol"), "trow"),
            P(("arcs", "tcol")),
            P(("arcs", "tcol")),
            P(("arcs", "tcol")),
        ),
        out_specs=(P("trow", ("arcs", "tcol")), P("trow")),
        check_vma=False,
    )
```

```python
import jax
import jax.numpy as jnp
from jax import lax
from jax.experimental import pallas as pl
from jax.experimental.pallas import tpu as pltpu
from jax.sharding import PartitionSpec as P


AXES = ("arcs", "trow", "tcol")
CHUNKS = 1
VMEM = pl.BlockSpec(memory_space=pltpu.VMEM)
SMEM = pl.BlockSpec(memory_space=pltpu.SMEM)


def device_index(x, y, core, zh, zl):
    return (zl * 8 + y * 2 + core) * 16 + x * 4 + zh


def moved(value, where):
    pairs = []
    for x in range(4):
        for y in range(4):
            for core in range(2):
                for zh in range(4):
                    for zl in range(2):
                        pairs.append(
                            (device_index(x, y, core, zh, zl), device_index(*where(x, y, core, zh, zl)))
                        )
    return lax.ppermute(value, AXES, pairs)


def along_z(step):
    def where(x, y, core, zh, zl):
        z = (zh * 2 + zl + step) % 8
        return x, y, core, z // 2, z % 2

    return where


def round_y(x, y, core, zh, zl):
    return x, (y + (1 if core == 0 else 3)) % 4, core, zh, zl


def other_core(x, y, core, zh, zl):
    return x, y, 1 - core, zh, zl


def first_x(x, y, core, zh, zl):
    return x ^ (1 if core == 0 else 3), y, core, zh, zl


def second_x(x, y, core, zh, zl):
    return x ^ (3 if core == 0 else 1), y, core, zh, zl


def flip_z(mask):
    def where(x, y, core, zh, zl):
        z = (zh * 2 + zl) ^ mask
        return x, y, core, z // 2, z % 2

    return where


def to_share(turn):
    def where(x, y, core, zh, zl):
        a = y // 2
        return x, (y if zl == a else 3 - y), core, (zh + turn) % 4, a

    return where


def centre(where_ref, design_ref, small_ref, *refs):
    chunk_refs, share_refs = refs[:CHUNKS], refs[CHUNKS : CHUNKS + 4]
    rhs_ref, out_ref = refs[CHUNKS + 4 :]
    rows, cols = design_ref.shape
    arcs = (small_ref.shape[1] - rows) // 2
    length = rows // arcs
    slot = lax.broadcasted_iota(jnp.int32, (length, 1), 0).astype(jnp.float32)
    lane = lax.broadcasted_iota(jnp.int32, (1, rows), 1).astype(jnp.float32)
    observed = small_ref[:, :rows]
    weighted = jnp.zeros((1, rows), jnp.float32)
    for arc in range(arcs):
        root = jnp.sqrt(small_ref[:, rows + arc : rows + arc + 1])
        count = small_ref[:, rows + arcs + arc : rows + arcs + arc + 1]
        mask = (slot < count).astype(jnp.float32)
        piece = design_ref[pl.ds(arc * length, length), :].astype(jnp.float32)
        mean = jnp.sum(mask * piece, axis=0, keepdims=True) / count
        out_ref[pl.ds(arc * length, length), :] = ((mask * root) * (piece - mean)).astype(jnp.bfloat16)
        inside = ((lane >= arc * length) & (lane < arc * length + count)).astype(jnp.float32)
        series_mean = jnp.sum(inside * observed, axis=1, keepdims=True) / count
        weighted = weighted + (inside * root) * (observed - series_mean)
    high = weighted.astype(jnp.bfloat16)
    rest1 = weighted - high.astype(jnp.float32)
    middle = rest1.astype(jnp.bfloat16)
    low = (rest1 - middle.astype(jnp.float32)).astype(jnp.bfloat16)
    row = lax.broadcasted_iota(jnp.int32, (8, rows), 0)
    parts = jnp.where(
        row == 0,
        high.astype(jnp.float32),
        jnp.where(row == 1, middle.astype(jnp.float32), jnp.where(row == 2, low.astype(jnp.float32), 0.0)),
    ).astype(jnp.bfloat16)
    sums = jnp.dot(parts, out_ref[...], preferred_element_type=jnp.float32)
    rhs_ref[...] = jnp.sum(sums, axis=0, keepdims=True)
    narrow = cols // 4
    for turn, share_ref in enumerate(share_refs):
        start = pl.multiple_of(((where_ref[3] + turn) % 4) * narrow, 128)
        share_ref[...] = out_ref[:, pl.ds(start, narrow)]
    wide = cols // CHUNKS
    for c, chunk_ref in enumerate(chunk_refs):
        chunk_ref[...] = out_ref[:, c * wide : (c + 1) * wide]


def joined(columns):
    rows = sum(piece.shape[0] for piece in columns[0])
    wide = sum(pieces[0].shape[-1] for pieces in columns)

    def join(*refs):
        refs, out_ref, left = iter(refs[:-1]), refs[-1], 0
        for pieces in columns:
            top = 0
            for piece in pieces:
                spot = (pl.ds(top, piece.shape[0]),) + (slice(None),) * (piece.ndim - 2)
                out_ref[spot + (pl.ds(left, piece.shape[-1]),)] = next(refs)[...]
                top += piece.shape[0]
            left += pieces[0].shape[-1]

    flat = [piece for pieces in columns for piece in pieces]
    return pl.pallas_call(
        join,
        out_shape=jax.ShapeDtypeStruct((rows, *flat[0].shape[1:-1], wide), flat[0].dtype),
        in_specs=[VMEM] * len(flat),
        out_specs=VMEM,
        compiler_params=pltpu.CompilerParams(vmem_limit_bytes=12 << 20),
    )(*flat)


def place(where_ref, mine_ref, theirs_ref, cols_out):
    x, y, core, zh, zl = (where_ref[i] for i in range(5))
    z = 2 * zh + zl
    first = jnp.where(core == 0, 1, 3)
    for other, ref in enumerate((mine_ref, theirs_ref)):
        source_core = (core + other) % 2
        for step in range(4):
            from_y = (y + jnp.where(source_core == 0, 4 - step, step)) % 4
            near = from_y // 2 == zl
            of_y = jnp.where(near, from_y, 3 - from_y)
            of_zl = jnp.where(near, zl, 1 - zl)
            m = (2 * (of_y % 2) + source_core) ^ x
            spot = jnp.where(m == 0, 0, jnp.where(m == 2, 3, jnp.where(m == first, 2, 1)))
            for turn in range(4):
                of_z = 2 * ((zh + 4 - turn) % 4) + of_zl
                ahead = (of_z + 8 - z) % 8
                cols_out[spot, pl.ds(pl.multiple_of(ahead * 128, 128), 128), :] = ref[4 * step + turn]


def product(left, right):
    return lax.dot_general(left, right, (((0,), (0,)), ((), ())), preferred_element_type=jnp.float32)


def local(design, observed, arc_counts, arc_weight):
    rows, cols = design.shape
    narrow = cols // 4
    obs_total = 4096
    bf16, f32 = jnp.bfloat16, jnp.float32
    trow, tcol = lax.axis_index("trow"), lax.axis_index("tcol")
    where = jnp.stack([tcol // 4, trow // 2, trow % 2, tcol % 4, lax.axis_index("arcs")])

    small = jnp.concatenate([observed, arc_weight, arc_counts.astype(f32)])
    out = pl.pallas_call(
        centre,
        out_shape=[jax.ShapeDtypeStruct((rows, cols // CHUNKS), bf16)] * CHUNKS
        + [jax.ShapeDtypeStruct((rows, narrow), bf16)] * 4
        + [jax.ShapeDtypeStruct((1, cols), f32)],
        in_specs=[SMEM, VMEM, VMEM],
        out_specs=[VMEM] * (CHUNKS + 5),
        scratch_shapes=[pltpu.VMEM((rows, cols), bf16)],
        compiler_params=pltpu.CompilerParams(vmem_limit_bytes=8 << 20),
        name="centre",
    )(where, design, small.reshape(1, -1))
    own, shares, rhs = out[:CHUNKS], out[CHUNKS:-1], out[-1].reshape(cols)

    mine = [jnp.concatenate([moved(shares[turn], to_share(turn))[None] for turn in range(4)])]
    for _ in range(1, 4):
        mine.append(moved(mine[-1], round_y))
    mine = joined([mine])
    theirs = moved(mine, other_core)
    right = pl.pallas_call(
        place,
        out_shape=jax.ShapeDtypeStruct((4, 8 * rows, narrow), bf16),
        in_specs=[SMEM, VMEM, VMEM],
        out_specs=VMEM,
        compiler_params=pltpu.CompilerParams(vmem_limit_bytes=12 << 20),
        name="place",
    )(where, mine, theirs)

    half = rows // 2
    columns = []
    for piece in own:
        up, down = [piece], [piece]
        for _ in range(1, 4):
            up.append(moved(up[-1], along_z(1)))
            down.append(moved(down[-1], along_z(-1)))
        far = [moved(up[3][:half], along_z(1)), moved(down[3][half:], along_z(-1))]
        columns.append([piece, *down[1:], *far, up[3], up[2], up[1]])
    left = joined(columns)

    far = moved(product(left, right[3]).astype(bf16), first_x)
    near = moved(product(left, right[2]).astype(bf16), first_x)
    second, tile = lax.optimization_barrier((product(left, right[1]), product(left, right[0])))
    last = moved((second + far.astype(f32)).astype(bf16), second_x)
    gram = (tile + near.astype(f32) + last.astype(f32)) * (1.0 / obs_total)

    rhs = rhs + moved(rhs, first_x)
    rhs = rhs + moved(rhs, second_x)
    for mask in (1, 2, 4):
        rhs = rhs + moved(rhs, flip_z(mask))
    return (gram, rhs * obs_total ** (-0.5))


def solution(mesh):
    return jax.shard_map(
        local,
        mesh=mesh,
        in_specs=(
            P(("arcs", "tcol"), "trow"),
            P(("arcs", "tcol")),
            P(("arcs", "tcol")),
            P(("arcs", "tcol")),
        ),
        out_specs=(P("trow", ("arcs", "tcol")), P("trow")),
        check_vma=False,
    )
```

```python
import jax
import jax.numpy as jnp
from jax import lax
from jax.experimental import pallas as pl
from jax.experimental.pallas import tpu as pltpu
from jax.sharding import PartitionSpec as P


AXES = ("arcs", "trow", "tcol")
VMEM = pl.BlockSpec(memory_space=pltpu.VMEM)
SMEM = pl.BlockSpec(memory_space=pltpu.SMEM)


def device_index(x, y, core, zh, zl):
    return (zl * 8 + y * 2 + core) * 16 + x * 4 + zh


def moved(value, where):
    pairs = []
    for x in range(4):
        for y in range(4):
            for core in range(2):
                for zh in range(4):
                    for zl in range(2):
                        pairs.append(
                            (device_index(x, y, core, zh, zl), device_index(*where(x, y, core, zh, zl)))
                        )
    return lax.ppermute(value, AXES, pairs)


def along_z(step):
    def where(x, y, core, zh, zl):
        z = (zh * 2 + zl + step) % 8
        return x, y, core, z // 2, z % 2

    return where


def along_y(step):
    return lambda x, y, core, zh, zl: (x, (y + step) % 4, core, zh, zl)


def other_core(x, y, core, zh, zl):
    return x, y, 1 - core, zh, zl


def first_x(x, y, core, zh, zl):
    return x ^ (1 if core == 0 else 3), y, core, zh, zl


def second_x(x, y, core, zh, zl):
    return x ^ (3 if core == 0 else 1), y, core, zh, zl


def flip_z(mask):
    def where(x, y, core, zh, zl):
        z = (zh * 2 + zl) ^ mask
        return x, y, core, z // 2, z % 2

    return where


def across_y(x, y, core, zh, zl):
    return x, 3 - y, core, zh, zl


def handed(core_of_four, sign):
    def where(x, y, core, zh, zl):
        z = zh * 2 + zl
        if y // 2 == zl:
            z, y = (z + 2 * sign) % 8, 3 - y
        elif core == core_of_four:
            z = (z + 3 * sign) % 8
        else:
            y = 3 - y
        return x, y, core, z // 2, z % 2

    return where


def centre(where_ref, design_ref, small_ref, *refs):
    out_ref, rhs_ref = refs
    rows, _ = design_ref.shape
    arcs = (small_ref.shape[1] - rows) // 2
    length = rows // arcs
    slot = lax.broadcasted_iota(jnp.int32, (length, 1), 0).astype(jnp.float32)
    lane = lax.broadcasted_iota(jnp.int32, (1, rows), 1).astype(jnp.float32)
    observed = small_ref[:, :rows]
    weighted = jnp.zeros((1, rows), jnp.float32)
    for arc in range(arcs):
        root = jnp.sqrt(small_ref[:, rows + arc : rows + arc + 1])
        count = small_ref[:, rows + arcs + arc : rows + arcs + arc + 1]
        mask = (slot < count).astype(jnp.float32)
        piece = design_ref[pl.ds(arc * length, length), :].astype(jnp.float32)
        mean = jnp.sum(mask * piece, axis=0, keepdims=True) / count
        out_ref[pl.ds(arc * length, length), :] = ((mask * root) * (piece - mean)).astype(jnp.bfloat16)
        inside = ((lane >= arc * length) & (lane < arc * length + count)).astype(jnp.float32)
        series_mean = jnp.sum(inside * observed, axis=1, keepdims=True) / count
        weighted = weighted + (inside * root) * (observed - series_mean)
    high = weighted.astype(jnp.bfloat16)
    rest1 = weighted - high.astype(jnp.float32)
    middle = rest1.astype(jnp.bfloat16)
    low = (rest1 - middle.astype(jnp.float32)).astype(jnp.bfloat16)
    row = lax.broadcasted_iota(jnp.int32, (8, rows), 0)
    parts = jnp.where(
        row == 0,
        high.astype(jnp.float32),
        jnp.where(row == 1, middle.astype(jnp.float32), jnp.where(row == 2, low.astype(jnp.float32), 0.0)),
    ).astype(jnp.bfloat16)
    sums = jnp.dot(parts, out_ref[...], preferred_element_type=jnp.float32)
    rhs_ref[...] = jnp.sum(sums, axis=0, keepdims=True)


def pick(where_ref, first_ref, second_ref, out_ref):
    start = pl.multiple_of(where_ref[3] * out_ref.shape[2], 128)
    out_ref[0] = first_ref[:, pl.ds(start, out_ref.shape[2])]
    out_ref[1] = second_ref[:, pl.ds(start, out_ref.shape[2])]


def pick_for_others(where_ref, ahead_ref, behind_ref, first_ref, second_ref):
    y, zh, zl = where_ref[1], where_ref[3], where_ref[4]
    z, wide = 2 * zh + zl, first_ref.shape[1]
    links = jnp.where(y // 2 == zl, 2, 3)
    start = (z + 8 - links) % 8 // 2 * wide
    first_ref[...] = ahead_ref[:, pl.ds(pl.multiple_of(start, 128), wide)]
    start = (z + links) % 8 // 2 * wide
    second_ref[...] = behind_ref[:, pl.ds(pl.multiple_of(start, 128), wide)]


def make_share(where_ref, behind1_ref, ahead2_ref, behind2_ref, here_ref, first_ref, second_ref, out_ref):
    y, zh, zl = where_ref[1], where_ref[3], where_ref[4]
    wide = out_ref.shape[2]
    start = pl.multiple_of(zh * wide, 128)
    near = y // 2 == zl

    @pl.when(near)
    def _():
        out_ref[0] = behind1_ref[:, pl.ds(start, wide)]
        out_ref[1] = ahead2_ref[:, pl.ds(start, wide)]
        out_ref[2] = behind2_ref[:, pl.ds(start, wide)]

    @pl.when(near & (where_ref[2] == 0))
    def _():
        out_ref[3] = first_ref[...]

    @pl.when(near & (where_ref[2] == 1))
    def _():
        out_ref[3] = second_ref[...]

    @pl.when(jnp.logical_not(near))
    def _():
        out_ref[0] = here_ref[0]
        out_ref[1] = here_ref[1]
        out_ref[2] = first_ref[...]
        out_ref[3] = second_ref[...]


def joined(columns):
    rows = sum(piece.shape[0] for piece in columns[0])
    wide = sum(pieces[0].shape[-1] for pieces in columns)

    def join(*refs):
        refs, out_ref, left = iter(refs[:-1]), refs[-1], 0
        for pieces in columns:
            top = 0
            for piece in pieces:
                spot = (pl.ds(top, piece.shape[0]),) + (slice(None),) * (piece.ndim - 2)
                out_ref[spot + (pl.ds(left, piece.shape[-1]),)] = next(refs)[...]
                top += piece.shape[0]
            left += pieces[0].shape[-1]

    flat = [piece for pieces in columns for piece in pieces]
    return pl.pallas_call(
        join,
        out_shape=jax.ShapeDtypeStruct((rows, *flat[0].shape[1:-1], wide), flat[0].dtype),
        in_specs=[VMEM] * len(flat),
        out_specs=VMEM,
        compiler_params=pltpu.CompilerParams(vmem_limit_bytes=12 << 20),
    )(*flat)


def place(where_ref, *refs):
    refs, cols_out = refs[:-1], refs[-1]
    x, y, core, _, zl = (where_ref[i] for i in range(5))
    first = jnp.where(core == 0, 1, 3)

    def put(source_core, offset, turn, ref, row):
        from_y = (y + offset) % 4
        near = from_y // 2 == zl
        of_y = jnp.where(near, from_y, 3 - from_y)
        m = (2 * (of_y % 2) + source_core) ^ x
        spot = jnp.where(m == 0, 0, jnp.where(m == 2, 3, jnp.where(m == first, 2, 1)))
        ahead = jnp.where(near, (7, 2, 6, 4)[turn], (0, 1, 3, 5)[turn])
        cols_out[spot, pl.ds(pl.multiple_of(ahead * 128, 128), 128), :] = ref[row]

    for other in range(2):
        source_core = (core + other) % 2
        near_ref, far_ref = refs[2 * other : 2 * other + 2]
        for turn in range(4):
            for step, offset in enumerate((0, 3, 1)):
                put(source_core, offset, turn, near_ref, 4 * step + turn)
            put(source_core, 2, turn, far_ref, turn)


def product(left, right):
    return lax.dot_general(left, right, (((0,), (0,)), ((), ())), preferred_element_type=jnp.float32)


def local(design, observed, arc_counts, arc_weight):
    rows, cols = design.shape
    narrow = cols // 4
    obs_total = 4096
    bf16, f32 = jnp.bfloat16, jnp.float32
    trow, tcol = lax.axis_index("trow"), lax.axis_index("tcol")
    where = jnp.stack([tcol // 4, trow // 2, trow % 2, tcol % 4, lax.axis_index("arcs")])

    small = jnp.concatenate([observed, arc_weight, arc_counts.astype(f32)])
    centered, rhs = pl.pallas_call(
        centre,
        out_shape=[jax.ShapeDtypeStruct((rows, cols), bf16), jax.ShapeDtypeStruct((1, cols), f32)],
        in_specs=[SMEM, VMEM, VMEM],
        out_specs=[VMEM] * 2,
        compiler_params=pltpu.CompilerParams(vmem_limit_bytes=8 << 20),
        name="centre",
    )(where, design, small.reshape(1, -1))
    rhs = rhs.reshape(cols)

    up, down = [centered], [centered]
    for _ in range(1, 4):
        up.append(moved(up[-1], along_z(1)))
        down.append(moved(down[-1], along_z(-1)))
    half = rows // 2
    far = [moved(up[3][:half], along_z(1)), moved(down[3][half:], along_z(-1))]
    left = joined([[centered, *down[1:], *far, up[3], up[2], up[1]]])

    def small_call(kernel, pieces, *shapes):
        return pl.pallas_call(
            kernel,
            out_shape=[jax.ShapeDtypeStruct(shape, bf16) for shape in shapes],
            in_specs=[SMEM] + [VMEM] * len(pieces),
            out_specs=[VMEM] * len(shapes),
            compiler_params=pltpu.CompilerParams(vmem_limit_bytes=8 << 20),
        )(where, *pieces)

    (here,) = small_call(pick, [centered, down[1]], (2, rows, narrow))
    here = moved(here, across_y)
    first, second = small_call(pick_for_others, [down[1], up[1]], (rows, narrow), (rows, narrow))
    first, second = moved(first, handed(0, -1)), moved(second, handed(1, 1))
    (share,) = small_call(
        make_share, [up[1], down[2], up[2], here, first, second], (4, rows, narrow)
    )
    y1u, y1d = moved(share, along_y(1)), moved(share, along_y(-1))
    y2u, y2d = moved(y1u[:2], along_y(1)), moved(y1d[2:], along_y(-1))
    mine = [joined([[share, y1u, y1d]]), joined([[y2u, y2d]])]
    theirs = [moved(part, other_core) for part in mine]
    right = pl.pallas_call(
        place,
        out_shape=jax.ShapeDtypeStruct((4, 8 * rows, narrow), bf16),
        in_specs=[SMEM] + [VMEM] * 4,
        out_specs=VMEM,
        compiler_params=pltpu.CompilerParams(vmem_limit_bytes=12 << 20),
        name="place",
    )(where, *mine, *theirs)

    far = moved(product(left, right[3]).astype(bf16), first_x)
    near = moved(product(left, right[2]).astype(bf16), first_x)
    second, tile = lax.optimization_barrier((product(left, right[1]), product(left, right[0])))
    last = moved((second + far.astype(f32)).astype(bf16), second_x)
    gram = (tile + near.astype(f32) + last.astype(f32)) * (1.0 / obs_total)

    rhs = rhs + moved(rhs, first_x)
    rhs = rhs + moved(rhs, second_x)
    for mask in (1, 2, 4):
        rhs = rhs + moved(rhs, flip_z(mask))
    return (gram, rhs * obs_total ** (-0.5))


def solution(mesh):
    return jax.shard_map(
        local,
        mesh=mesh,
        in_specs=(
            P(("arcs", "tcol"), "trow"),
            P(("arcs", "tcol")),
            P(("arcs", "tcol")),
            P(("arcs", "tcol")),
        ),
        out_specs=(P("trow", ("arcs", "tcol")), P("trow")),
        check_vma=False,
    )
```

```python
from functools import partial

import jax
import jax.numpy as jnp
from jax import lax
from jax.experimental import pallas as pl
from jax.experimental.pallas import tpu as pltpu
from jax.sharding import PartitionSpec as P


AXES = ("arcs", "trow", "tcol")
VMEM = pl.BlockSpec(memory_space=pltpu.VMEM)
SMEM = pl.BlockSpec(memory_space=pltpu.SMEM)


def device_index(x, y, core, zh, zl):
    return (zl * 8 + y * 2 + core) * 16 + x * 4 + zh


def moved(value, where):
    pairs = []
    for x in range(4):
        for y in range(4):
            for core in range(2):
                for zh in range(4):
                    for zl in range(2):
                        pairs.append(
                            (device_index(x, y, core, zh, zl), device_index(*where(x, y, core, zh, zl)))
                        )
    return lax.ppermute(value, AXES, pairs)


def along_z(step):
    def where(x, y, core, zh, zl):
        z = (zh * 2 + zl + step) % 8
        return x, y, core, z // 2, z % 2

    return where


def along_y(step):
    return lambda x, y, core, zh, zl: (x, (y + step) % 4, core, zh, zl)


def other_core(x, y, core, zh, zl):
    return x, y, 1 - core, zh, zl


def first_x(x, y, core, zh, zl):
    return x ^ (1 if core == 0 else 3), y, core, zh, zl


def second_x(x, y, core, zh, zl):
    return x ^ (3 if core == 0 else 1), y, core, zh, zl


def flip_z(mask):
    def where(x, y, core, zh, zl):
        z = (zh * 2 + zl) ^ mask
        return x, y, core, z // 2, z % 2

    return where


def across_y(x, y, core, zh, zl):
    return x, 3 - y, core, zh, zl


def handed(core_of_four, sign):
    def where(x, y, core, zh, zl):
        z = zh * 2 + zl
        if y // 2 == zl:
            z, y = (z + 2 * sign) % 8, 3 - y
        elif core == core_of_four:
            z = (z + 3 * sign) % 8
        else:
            y = 3 - y
        return x, y, core, z // 2, z % 2

    return where


def centre(where_ref, design_ref, small_ref, *refs):
    out_ref, rhs_ref = refs
    rows, _ = design_ref.shape
    arcs = (small_ref.shape[1] - rows) // 2
    length = rows // arcs
    slot = lax.broadcasted_iota(jnp.int32, (length, 1), 0).astype(jnp.float32)
    lane = lax.broadcasted_iota(jnp.int32, (1, rows), 1).astype(jnp.float32)
    observed = small_ref[:, :rows]
    weighted = jnp.zeros((1, rows), jnp.float32)
    for arc in range(arcs):
        root = jnp.sqrt(small_ref[:, rows + arc : rows + arc + 1])
        count = small_ref[:, rows + arcs + arc : rows + arcs + arc + 1]
        mask = (slot < count).astype(jnp.float32)
        piece = design_ref[pl.ds(arc * length, length), :].astype(jnp.float32)
        mean = jnp.sum(mask * piece, axis=0, keepdims=True) / count
        out_ref[pl.ds(arc * length, length), :] = ((mask * root) * (piece - mean)).astype(jnp.bfloat16)
        inside = ((lane >= arc * length) & (lane < arc * length + count)).astype(jnp.float32)
        series_mean = jnp.sum(inside * observed, axis=1, keepdims=True) / count
        weighted = weighted + (inside * root) * (observed - series_mean)
    high = weighted.astype(jnp.bfloat16)
    rest1 = weighted - high.astype(jnp.float32)
    middle = rest1.astype(jnp.bfloat16)
    low = (rest1 - middle.astype(jnp.float32)).astype(jnp.bfloat16)
    row = lax.broadcasted_iota(jnp.int32, (8, rows), 0)
    parts = jnp.where(
        row == 0,
        high.astype(jnp.float32),
        jnp.where(row == 1, middle.astype(jnp.float32), jnp.where(row == 2, low.astype(jnp.float32), 0.0)),
    ).astype(jnp.bfloat16)
    sums = jnp.dot(parts, out_ref[...], preferred_element_type=jnp.float32)
    rhs_ref[...] = jnp.sum(sums, axis=0, keepdims=True)


def pick(where_ref, first_ref, second_ref, out_ref):
    start = pl.multiple_of(where_ref[3] * out_ref.shape[2], 128)
    out_ref[0] = first_ref[:, pl.ds(start, out_ref.shape[2])]
    out_ref[1] = second_ref[:, pl.ds(start, out_ref.shape[2])]


def pick_for_others(where_ref, ahead_ref, behind_ref, first_ref, second_ref):
    y, zh, zl = where_ref[1], where_ref[3], where_ref[4]
    z, wide = 2 * zh + zl, first_ref.shape[1]
    links = jnp.where(y // 2 == zl, 2, 3)
    start = (z + 8 - links) % 8 // 2 * wide
    first_ref[...] = ahead_ref[:, pl.ds(pl.multiple_of(start, 128), wide)]
    start = (z + links) % 8 // 2 * wide
    second_ref[...] = behind_ref[:, pl.ds(pl.multiple_of(start, 128), wide)]


def make_share(where_ref, behind1_ref, ahead2_ref, behind2_ref, here_ref, first_ref, second_ref, out_ref):
    y, zh, zl = where_ref[1], where_ref[3], where_ref[4]
    wide = out_ref.shape[2]
    start = pl.multiple_of(zh * wide, 128)
    near = y // 2 == zl

    @pl.when(near)
    def _():
        out_ref[0] = behind1_ref[:, pl.ds(start, wide)]
        out_ref[1] = ahead2_ref[:, pl.ds(start, wide)]
        out_ref[2] = behind2_ref[:, pl.ds(start, wide)]

    @pl.when(near & (where_ref[2] == 0))
    def _():
        out_ref[3] = first_ref[...]

    @pl.when(near & (where_ref[2] == 1))
    def _():
        out_ref[3] = second_ref[...]

    @pl.when(jnp.logical_not(near))
    def _():
        out_ref[0] = here_ref[0]
        out_ref[1] = here_ref[1]
        out_ref[2] = first_ref[...]
        out_ref[3] = second_ref[...]


def joined(columns):
    rows = sum(piece.shape[0] for piece in columns[0])
    wide = sum(pieces[0].shape[-1] for pieces in columns)

    def join(*refs):
        refs, out_ref, left = iter(refs[:-1]), refs[-1], 0
        for pieces in columns:
            top = 0
            for piece in pieces:
                spot = (pl.ds(top, piece.shape[0]),) + (slice(None),) * (piece.ndim - 2)
                out_ref[spot + (pl.ds(left, piece.shape[-1]),)] = next(refs)[...]
                top += piece.shape[0]
            left += pieces[0].shape[-1]

    flat = [piece for pieces in columns for piece in pieces]
    return pl.pallas_call(
        join,
        out_shape=jax.ShapeDtypeStruct((rows, *flat[0].shape[1:-1], wide), flat[0].dtype),
        in_specs=[VMEM] * len(flat),
        out_specs=VMEM,
        compiler_params=pltpu.CompilerParams(vmem_limit_bytes=12 << 20),
    )(*flat)


def place(parts, where_ref, *refs):
    cols_out = refs[-1]
    x, y, core, _, zl = (where_ref[i] for i in range(5))
    first = jnp.where(core == 0, 1, 3)

    def put(source_core, offset, turn, ref, row):
        from_y = (y + offset) % 4
        near = from_y // 2 == zl
        of_y = jnp.where(near, from_y, 3 - from_y)
        m = (2 * (of_y % 2) + source_core) ^ x
        spot = jnp.where(m == 0, 0, jnp.where(m == 2, 3, jnp.where(m == first, 2, 1)))
        ahead = jnp.where(near, (7, 2, 6, 4)[turn], (0, 1, 3, 5)[turn])
        cols_out[spot, pl.ds(pl.multiple_of(ahead * 128, 128), 128), :] = ref[row]

    for (other, offsets), ref in zip(parts, refs):
        for step, offset in enumerate(offsets):
            for turn in range(4):
                put((core + other) % 2, offset, turn, ref, 4 * step + turn)


def product(left, right):
    return lax.dot_general(left, right, (((0,), (0,)), ((), ())), preferred_element_type=jnp.float32)


def local(design, observed, arc_counts, arc_weight):
    rows, cols = design.shape
    narrow = cols // 4
    obs_total = 4096
    bf16, f32 = jnp.bfloat16, jnp.float32
    trow, tcol = lax.axis_index("trow"), lax.axis_index("tcol")
    where = jnp.stack([tcol // 4, trow // 2, trow % 2, tcol % 4, lax.axis_index("arcs")])

    arcs = arc_counts.shape[0]
    small = (
        jnp.pad(observed, (0, 2 * arcs))
        + jnp.pad(arc_weight, (rows, arcs))
        + jnp.pad(arc_counts.astype(f32), (rows + arcs, 0))
    )
    centered, rhs = pl.pallas_call(
        centre,
        out_shape=[jax.ShapeDtypeStruct((rows, cols), bf16), jax.ShapeDtypeStruct((1, cols), f32)],
        in_specs=[SMEM, VMEM, VMEM],
        out_specs=[VMEM] * 2,
        compiler_params=pltpu.CompilerParams(vmem_limit_bytes=8 << 20),
        name="centre",
    )(where, design, small.reshape(1, -1))
    rhs = rhs.reshape(cols)

    up, down = [centered], [centered]
    for _ in range(1, 4):
        up.append(moved(up[-1], along_z(1)))
        down.append(moved(down[-1], along_z(-1)))
    half = rows // 2
    far = [moved(up[3][:half], along_z(1)), moved(down[3][half:], along_z(-1))]
    left = joined([[centered, *down[1:], *far, up[3], up[2], up[1]]])

    def small_call(kernel, pieces, *shapes):
        return pl.pallas_call(
            kernel,
            out_shape=[jax.ShapeDtypeStruct(shape, bf16) for shape in shapes],
            in_specs=[SMEM] + [VMEM] * len(pieces),
            out_specs=[VMEM] * len(shapes),
            compiler_params=pltpu.CompilerParams(vmem_limit_bytes=8 << 20),
        )(where, *pieces)

    (here,) = small_call(pick, [centered, down[1]], (2, rows, narrow))
    here = moved(here, across_y)
    first, second = small_call(pick_for_others, [down[1], up[1]], (rows, narrow), (rows, narrow))
    first, second = moved(first, handed(0, -1)), moved(second, handed(1, 1))
    (share,) = small_call(
        make_share, [up[1], down[2], up[2], here, first, second], (4, rows, narrow)
    )
    y1u, y1d = moved(share, along_y(1)), moved(share, along_y(-1))
    y2u, y2d = moved(y1u[:2], along_y(1)), moved(y1d[2:], along_y(-1))
    mine = [joined([[share, y1u, y1d]]), joined([[y2u, y2d]])]
    theirs = [moved(part, other_core) for part in mine]

    def placed(parts, pieces, before=()):
        return pl.pallas_call(
            partial(place, parts),
            out_shape=jax.ShapeDtypeStruct((4, 8 * rows, narrow), bf16),
            in_specs=[SMEM] + [VMEM] * (len(pieces) + len(before)),
            out_specs=VMEM,
            input_output_aliases={1 + len(pieces): 0} if before else {},
            compiler_params=pltpu.CompilerParams(vmem_limit_bytes=12 << 20),
        )(where, *pieces, *before)

    close, across = (0, 3, 1), (2,)
    right = placed(((0, close), (0, across), (1, close)), (*mine, theirs[0]))
    right = placed(((1, across),), theirs[1:], (right,))

    far = moved(product(left, right[3]).astype(bf16), first_x)
    near = moved(product(left, right[2]).astype(bf16), first_x)
    second, tile = lax.optimization_barrier((product(left, right[1]), product(left, right[0])))
    last = moved((second + far.astype(f32)).astype(bf16), second_x)
    tile = lax.optimization_barrier(tile + near.astype(f32))
    gram = (tile + last.astype(f32)) * (1.0 / obs_total)

    rhs = rhs + moved(rhs, first_x)
    rhs = rhs + moved(rhs, second_x)
    for mask in (1, 2, 4):
        rhs = rhs + moved(rhs, flip_z(mask))
    return (gram, rhs * obs_total ** (-0.5))


def solution(mesh):
    return jax.shard_map(
        local,
        mesh=mesh,
        in_specs=(
            P(("arcs", "tcol"), "trow"),
            P(("arcs", "tcol")),
            P(("arcs", "tcol")),
            P(("arcs", "tcol")),
        ),
        out_specs=(P("trow", ("arcs", "tcol")), P("trow")),
        check_vma=False,
    )
```
